32 devices in a mesh: sa: 4 (over y, core), sb: 8 (over z, x).
Axes of the slice: x: 2, y: 2, z: 4, core: 2. Of those that a mesh axis runs over, the one named last changes fastest.
Arguments:
- queries: bfloat16 [1024, 1024], P(('sa', 'sb')), may hold values from -6 to 6
- out_grad: bfloat16 [1024, 1024], P(('sa', 'sb')), may hold values from -6144 to 6144
- forward_out: bfloat16 [1024, 1024], P(('sa', 'sb')), may hold values from -3 to 3
- lse_shift: float32 [1024, 8], P(('sa', 'sb')), may hold values from 0.2 to 1
- key_rows: bfloat16 [32768, 256], P(('sa', 'sb')), may hold values from -7 to 7
- value_rows: bfloat16 [32768, 256], P(('sa', 'sb')), may hold values from -6 to 6
Outputs:
- query_grad: float32 [1024, 1024], P(('sa', 'sb'))
- key_grad: bfloat16 [32768, 256], P(('sa', 'sb'))
- value_grad: bfloat16 [32768, 256], P(('sa', 'sb'))
The draws below stay inside these ranges and needn't reach their ends.
All inputs are finite; a program needn't handle non-finite values.
Results may differ from the reference program's by a relative error of at most 0.0097.
Values may be sent and summed in bfloat16 or wider, within the bound.
A program may use at most 64 MiB of HBM per device.

```python
import math
import jax
import jax.numpy as jnp
from jax import lax

QH = 8
KVH = 2
HEAD_DIM = 128
Q_ROWS = 1024
KEYS = 32768


def draw_key_rows(key, part):
    noise_key, offset_key = jax.random.split(jax.random.fold_in(key, 11))
    noise = jnp.clip(jax.random.normal(noise_key, (KEYS, KVH * HEAD_DIM), jnp.float32), -4.0, 4.0)
    offset = jax.random.uniform(offset_key, (KVH * HEAD_DIM,), jnp.float32, -1.0, 1.0)
    ramp = 1.0 + 2.0 * jnp.arange(KEYS, dtype=jnp.float32) / KEYS
    return (noise + ramp[:, None] * offset[None, :]).astype(jnp.bfloat16)


def levels(key, extent, shards, low, high):
    def one(axis_at, shards_of):
        draws = jax.random.uniform(jax.random.fold_in(jax.random.fold_in(key, 6), axis_at), (shards_of,), jnp.float32, low / len(shards), high / len(shards))
        return jnp.repeat(jnp.exp(draws), extent[axis_at] // shards_of).reshape((-1,) + (1,) * (len(extent) - axis_at - 1))

    factor_of = one(*shards[0])
    for cut in shards[1:]:
        factor_of = factor_of * one(*cut)
    return factor_of


def scatter_about(stream_key, dims, scale, bound, cuts=(), held_as=jnp.bfloat16):
    result = jax.random.normal(stream_key, dims, jnp.float32) * scale
    if len(cuts) > 0:
        result = levels(stream_key, dims, cuts, -0.22, 0.18) * result
    return jnp.clip(result, min=-bound, max=bound).astype(held_as)


def setup_inputs(seed: int = 0) -> dict:
    streams_of = jax.random.split(jax.random.key(seed), 7)
    return {
        "queries": scatter_about(streams_of[0], (Q_ROWS, QH * HEAD_DIM), 1.0, 6.0, ((0, 32),)),
        "out_grad": scatter_about(streams_of[1], (Q_ROWS, QH * HEAD_DIM), 1024.0, 6144.0, ((0, 32),)),
        "forward_out": scatter_about(streams_of[2], (Q_ROWS, QH * HEAD_DIM), 0.5, 3.0, ((0, 32),)),
        "lse_shift": jnp.clip(0.2 + 0.8 * jax.random.uniform(streams_of[3], (Q_ROWS, QH), jnp.float32) ** levels(streams_of[3], (Q_ROWS, QH), ((0, 32),), -0.2, 0.2), 0.2, 1.0),
        "key_rows": draw_key_rows(jax.random.fold_in(streams_of[6], 71), 0),
        "value_rows": scatter_about(streams_of[5], (KEYS, KVH * HEAD_DIM), 1.0, 6.0, ((0, 32),)),
    }


def reference(queries, out_grad, forward_out, lse_shift, key_rows, value_rows):
    per_group = QH // KVH
    score_scale = 1.0 / math.sqrt(HEAD_DIM)
    key_mean = lax.optimization_barrier(jnp.sum(key_rows.astype(jnp.float32), axis=0)) / KEYS
    smoothed = (key_rows.astype(jnp.float32) - key_mean).astype(jnp.bfloat16)
    query_full = queries.astype(jnp.float32).reshape(Q_ROWS, KVH, per_group, HEAD_DIM)
    grad_full = out_grad.astype(jnp.float32).reshape(Q_ROWS, KVH, per_group, HEAD_DIM)
    product = out_grad.astype(jnp.float32) * forward_out.astype(jnp.float32)
    delta_rows = lax.optimization_barrier(jnp.sum(product.reshape(Q_ROWS, QH, HEAD_DIM), axis=-1))
    delta_heads = delta_rows.reshape(Q_ROWS, KVH, per_group).transpose(1, 2, 0)[..., None]
    offset_rows = lse_shift + math.log(KEYS)
    offset_heads = offset_rows.reshape(Q_ROWS, KVH, per_group).transpose(1, 2, 0)[..., None]
    key_block = 4096 if KEYS % 4096 == 0 else KEYS
    blocks = KEYS // key_block
    key_blocks = smoothed.reshape(blocks, key_block, KVH, HEAD_DIM)
    value_blocks = value_rows.reshape(blocks, key_block, KVH, HEAD_DIM)

    def block_step(query_acc, pieces):
        key_part = pieces[0].astype(jnp.float32)
        value_part = pieces[1].astype(jnp.float32)
        scores = jnp.einsum('qcgd,kcd->cgqk', query_full, key_part) * score_scale
        prob = jnp.exp(scores - offset_heads)
        prob_low = lax.optimization_barrier(prob.astype(jnp.bfloat16)).astype(jnp.float32)
        value_part_grad = jnp.einsum('cgqk,qcgd->kcd', prob_low, grad_full)
        dprob = jnp.einsum('qcgd,kcd->cgqk', grad_full, value_part)
        dscore = lax.optimization_barrier((prob * (dprob - delta_heads)).astype(jnp.bfloat16)).astype(jnp.float32)
        key_part_grad = jnp.einsum('cgqk,qcgd->kcd', dscore, query_full) * score_scale
        query_acc = query_acc + jnp.einsum('cgqk,kcd->qcgd', dscore, key_part) * score_scale
        return (query_acc, (key_part_grad.astype(jnp.bfloat16), value_part_grad.astype(jnp.bfloat16)))
    start = jnp.zeros((Q_ROWS, KVH, per_group, HEAD_DIM), jnp.float32)
    query_acc, outputs = lax.scan(block_step, start, (key_blocks, value_blocks))
    key_grad = outputs[0].reshape(KEYS, KVH * HEAD_DIM)
    value_grad = outputs[1].reshape(KEYS, KVH * HEAD_DIM)
    return (query_acc.reshape(Q_ROWS, QH * HEAD_DIM), key_grad, value_grad)
```

```python
import functools
import math

import jax
import jax.numpy as jnp
from jax import lax
from jax.experimental import pallas as pl
from jax.experimental.pallas import tpu as pltpu
from jax.sharding import PartitionSpec as P

QH = 8
KVH = 2
HEAD_DIM = 128
MESH = pl.DeviceIdType.MESH
BF = jnp.bfloat16
F32 = jnp.float32
AXES = ("sa", "sb")


def grid_of(sa, sb):
    inner = 2 ** (int(math.log2(sb)) // 2)
    return sa // 2, sb // inner, inner


class Place:
    def __init__(self, dims):
        self.dims = dims
        sa, sb = lax.axis_index("sa"), lax.axis_index("sb")
        self.core = sa % 2
        self.at = (sa // 2, sb // dims[2], sb % dims[2])

    def other(self, axis, step):
        at = list(self.at)
        at[axis] = (at[axis] + step) % self.dims[axis]
        return tuple(at)

    def back(self, offset):
        return tuple((p + n - o) % n for p, n, o in zip(self.at, self.dims, offset))

    def device(self, at):
        return (at[0] * 2 + self.core, at[1] * self.dims[2] + at[2])

    def partner(self):
        return (self.at[0] * 2 + 1 - self.core, lax.axis_index("sb"))

    def slot(self, at):
        return (at[0] * self.dims[1] + at[1]) * self.dims[2] + at[2]

    def greet(self):
        barrier = pltpu.get_barrier_semaphore()
        peers = [self.partner()]
        for axis in range(3):
            for step in range(1, self.dims[axis]):
                peers.append(self.device(self.other(axis, step)))
        for peer in peers:
            pl.semaphore_signal(barrier, inc=1, device_id=peer, device_id_type=MESH)
        pl.semaphore_wait(barrier, len(peers))


def pieces(x):
    hi = x.astype(BF)
    rest = x - hi.astype(F32)
    mid = rest.astype(BF)
    low = (rest - mid.astype(F32)).astype(BF)
    return hi, mid, low


def gather_sends(dims):
    na, nb, nd = dims
    sends = []
    for step in range(1, nb):
        sends.append(("qdx", (0, 0, 0), 1, step))
    for step in range(1, nd):
        sends.append(("qdx", (0, 0, 0), 2, step))
    for step in range(1, na):
        sends.append(("qdx", (0, 0, 0), 0, step))
    for b in range(1, nb):
        for step in range(1, nd):
            sends.append(("qdx", (0, b, 0), 2, step))
        for step in range(1, na):
            sends.append(("qdx", (0, b, 0), 0, step))
    for b in range(nb):
        for d in range(1, nd):
            for step in range(1, na):
                sends.append(("qx", (0, b, d), 0, step))
        for a in range(1, na):
            for step in range(1, nd):
                sends.append(("d", (a, b, 0), 2, step))
    return sends


def gather_kernel(dims, total_keys, q_ref, d_ref, o_ref, lse_ref, k_ref, v_ref,
                  qa_ref, da_ref, aux_ref, ks_ref, va_ref,
                  xa, kraw, half, halfr, send_sem, q_sem, d_sem, x_sem, kv_send, kv_recv):
    place = Place(dims)
    rows = q_ref.shape[0]
    keys = k_ref.shape[0]
    me = place.slot(place.at)
    scale = 1.0 / math.sqrt(HEAD_DIM)
    place.greet()

    def to_partner(src, dst, n):
        copy = pltpu.make_async_remote_copy(
            src_ref=src, dst_ref=dst, send_sem=kv_send.at[n], recv_sem=kv_recv.at[n],
            device_id=place.partner(), device_id_type=MESH)
        copy.start()
        return copy

    partner_copies = [to_partner(k_ref, kraw, 0), to_partner(v_ref, va_ref.at[1], 1)]

    bufs = {"q": (qa_ref, q_sem), "d": (da_ref, d_sem), "x": (xa, x_sem)}
    own = {"q": q_ref, "d": d_ref}
    started = []

    def flat(offset):
        return (offset[0] * dims[1] + offset[1]) * dims[2] + offset[2]

    def send(kind, offset, axis, step):
        buf, sem = bufs[kind]
        slot = place.slot(place.back(offset))
        src = own[kind] if kind in own and offset == (0, 0, 0) else buf.at[slot]
        there = list(offset)
        there[axis] = (there[axis] + step) % dims[axis]
        copy = pltpu.make_async_remote_copy(
            src_ref=src, dst_ref=buf.at[slot],
            send_sem=send_sem.at[len(started)], recv_sem=sem.at[flat(there)],
            device_id=place.device(place.other(axis, step)), device_id_type=MESH)
        copy.start()
        started.append(copy)

    arrived = set()

    def need(kind, offset):
        if offset == (0, 0, 0) or (kind, offset) in arrived:
            return
        arrived.add((kind, offset))
        buf, sem = bufs[kind]
        slot = place.slot(place.back(offset))
        pltpu.make_async_remote_copy(
            src_ref=buf.at[slot], dst_ref=buf.at[slot],
            send_sem=send_sem.at[0], recv_sem=sem.at[flat(offset)],
            device_id=place.partner(), device_id_type=MESH).wait_recv()

    sends = gather_sends(dims)
    first = [s for s in sends if s[1] == (0, 0, 0)]
    for kind in "qd":
        for kinds, offset, axis, step in first:
            if kind in kinds:
                send(kind, offset, axis, step)

    lane = lax.broadcasted_iota(jnp.int32, (rows, HEAD_DIM), 1)
    aux = jnp.zeros((rows, HEAD_DIM), F32)
    for head in range(QH):
        cols = pl.ds(head * HEAD_DIM, HEAD_DIM)
        product = d_ref[:, cols].astype(F32) * o_ref[:, cols].astype(F32)
        delta = jnp.sum(product, axis=1, keepdims=True)
        offset = (lse_ref[:, head:head + 1] + math.log(total_keys)) * (1.0 / scale)
        for at, value in ((0, offset), (3 * QH, delta)):
            for n, piece in enumerate(pieces(value)):
                aux = jnp.where(lane == at + 3 * head + n, piece.astype(F32), aux)
    xa[me, pl.ds(0, rows), :] = aux.astype(BF)
    chunk = 128

    def add_rows(n, acc):
        block = k_ref[pl.ds(pl.multiple_of(n * chunk, chunk), chunk), :].astype(F32)
        return acc + jnp.sum(block, axis=0, keepdims=True)

    key_sum = lax.fori_loop(0, keys // chunk, add_rows, jnp.zeros((1, KVH * HEAD_DIM), F32))
    row = lax.broadcasted_iota(jnp.int32, (16, HEAD_DIM), 0)
    small = jnp.zeros((16, HEAD_DIM), F32)
    for n, piece in enumerate(pieces(key_sum)):
        for c in range(KVH):
            part = piece[:, c * HEAD_DIM:(c + 1) * HEAD_DIM].astype(F32)
            small = jnp.where(row == 2 * n + c, part, small)
    xa[me, pl.ds(rows, 16), :] = small.astype(BF)
    for kinds, offset, axis, step in first:
        send("x", offset, axis, step)

    qa_ref[me] = q_ref[...]
    da_ref[me] = d_ref[...]
    va_ref[0] = v_ref[...]
    for kinds, offset, axis, step in sends:
        if offset == (0, 0, 0):
            continue
        for kind in kinds:
            need(kind, offset)
            send(kind, offset, axis, step)
    for a in range(dims[0]):
        for b in range(dims[1]):
            for d in range(dims[2]):
                for kind in "qdx":
                    need(kind, (a, b, d))

    members = dims[0] * dims[1] * dims[2]
    half_sum = jnp.zeros((16, HEAD_DIM), F32)
    for g in range(members):
        half_sum = half_sum + xa[g, pl.ds(rows, 16), :].astype(F32)
        aux_ref[pl.ds(g * rows, rows), :] = xa[g, pl.ds(0, rows), :]
    half[...] = half_sum
    partner_copies.append(to_partner(half, halfr, 2))
    for copy in partner_copies:
        copy.wait()
    both = half[...] + halfr[...]
    for c in range(KVH):
        cols = pl.ds(c * HEAD_DIM, HEAD_DIM)
        mean = (both[c:c + 1] + both[c + 2:c + 3] + both[c + 4:c + 5]) / total_keys

        def smooth(n, carry):
            at = pl.ds(pl.multiple_of(n * chunk, chunk), chunk)
            ks_ref[0, at, cols] = (k_ref[at, cols].astype(F32) - mean).astype(BF)
            ks_ref[1, at, cols] = (kraw[at, cols].astype(F32) - mean).astype(BF)
            return carry

        lax.fori_loop(0, keys // chunk, smooth, 0)
    for copy in started:
        copy.wait_send()


def gather(dims, total_keys, q, d, o, lse, k, v):
    members = dims[0] * dims[1] * dims[2]
    rows, width = q.shape
    keys, kw = k.shape
    count = sum(len(s[0]) for s in gather_sends(dims))
    vmem = pl.BlockSpec(memory_space=pltpu.VMEM)
    return pl.pallas_call(
        functools.partial(gather_kernel, dims, total_keys),
        name="gather",
        out_shape=(
            jax.ShapeDtypeStruct((members, rows, width), BF),
            jax.ShapeDtypeStruct((members, rows, width), BF),
            jax.ShapeDtypeStruct((members * rows, HEAD_DIM), BF),
            jax.ShapeDtypeStruct((2, keys, kw), BF),
            jax.ShapeDtypeStruct((2, keys, kw), BF),
        ),
        in_specs=[vmem] * 6,
        out_specs=(vmem,) * 5,
        scratch_shapes=[
            pltpu.VMEM((members, rows + 16, HEAD_DIM), BF),
            pltpu.VMEM((keys, kw), BF),
            pltpu.VMEM((16, HEAD_DIM), F32),
            pltpu.VMEM((16, HEAD_DIM), F32),
            pltpu.SemaphoreType.DMA((count,)),
            pltpu.SemaphoreType.DMA((members,)),
            pltpu.SemaphoreType.DMA((members,)),
            pltpu.SemaphoreType.DMA((members,)),
            pltpu.SemaphoreType.DMA((3,)),
            pltpu.SemaphoreType.DMA((3,)),
        ],
        compiler_params=pltpu.CompilerParams(collective_id=0, has_side_effects=True),
    )(q, d, o, lse, k, v)


def attend_kernel(q_ref, d_ref, aux_ref, k_ref, v_ref, dq_ref, dk_ref, dv_ref, acc):
    c, tile = pl.program_id(0), pl.program_id(1)
    per_group = QH // KVH
    scale = 1.0 / math.sqrt(HEAD_DIM)
    keys = k_ref[...]
    values = v_ref[...]
    aux = aux_ref[...]
    lane = lax.broadcasted_iota(jnp.int32, keys.shape, 1)
    nt = (((1,), (1,)), ((), ()))
    dk = jnp.zeros(keys.shape, F32)
    dv = jnp.zeros(keys.shape, F32)
    for g in range(per_group):
        head = c * per_group + g
        cols = pl.ds(g * HEAD_DIM, HEAD_DIM)
        heads_q = q_ref[:, cols]
        heads_d = d_ref[:, cols]
        at = 3 * head
        minus_s = jnp.where((lane >= at) & (lane < at + 3), -1.0, 0.0).astype(BF)
        at = 3 * QH + 3 * head
        minus_d = jnp.where((lane >= at) & (lane < at + 3), -1.0, 0.0).astype(BF)
        s = lax.dot_general(jnp.concatenate([keys, minus_s], 1),
                            jnp.concatenate([heads_q, aux], 1), nt,
                            preferred_element_type=F32)
        dp = lax.dot_general(jnp.concatenate([values, minus_d], 1),
                             jnp.concatenate([heads_d, aux], 1), nt,
                             preferred_element_type=F32)
        prob = jnp.exp2(s * (scale * math.log2(math.e)))
        dv = dv + jnp.dot(prob.astype(BF), heads_d, preferred_element_type=F32)
        ds = (prob * dp).astype(BF)
        dk = dk + jnp.dot(ds, heads_q, preferred_element_type=F32)
        dq = lax.dot_general(ds, keys, (((0,), (0,)), ((), ())), preferred_element_type=F32)

        @pl.when(tile == 0)
        def _():
            acc[:, cols] = dq

        @pl.when(tile > 0)
        def _():
            acc[:, cols] += dq

    dk_ref[...] = (dk * scale).astype(BF)
    dv_ref[...] = dv.astype(BF)

    @pl.when(tile == pl.num_programs(1) - 1)
    def _():
        dq_ref[...] = (acc[...] * scale).astype(BF)


def attend(q, d, aux, k, v, tile=512):
    rows, width = q.shape
    keys, kw = k.shape
    tile = min(tile, keys)
    group = width // KVH
    key_spec = pl.BlockSpec((tile, HEAD_DIM), lambda c, t: (t, c))
    row_spec = pl.BlockSpec((rows, group), lambda c, t: (0, c))
    return pl.pallas_call(
        attend_kernel,
        name="attend",
        grid=(KVH, keys // tile),
        out_shape=(
            jax.ShapeDtypeStruct((rows, width), BF),
            jax.ShapeDtypeStruct((keys, kw), BF),
            jax.ShapeDtypeStruct((keys, kw), BF),
        ),
        in_specs=[row_spec, row_spec, pl.BlockSpec((rows, HEAD_DIM), lambda c, t: (0, 0)),
                  key_spec, key_spec],
        out_specs=(row_spec, key_spec, key_spec),
        scratch_shapes=[pltpu.VMEM((rows, group), F32)],
        compiler_params=pltpu.CompilerParams(dimension_semantics=("arbitrary", "arbitrary")),
    )(q, d, aux, k, v)


def reduce_kernel(dims, p_ref, dk_ref, dv_ref, dq_out, dk_out, dv_out,
                  kvr, r1a, r1b, t1a, t1b, r2a, r2b, t2, r3, send_sem, recv_sem):
    na, nb, nd = dims
    place = Place(dims)
    a, b, d = place.at
    half = p_ref.shape[-1] // 2
    left, right = pl.ds(0, half), pl.ds(half, half)
    place.greet()
    copies = []

    def send(src, dst, device):
        n = len(copies)
        copy = pltpu.make_async_remote_copy(
            src_ref=src, dst_ref=dst, send_sem=send_sem.at[n], recv_sem=recv_sem.at[n],
            device_id=device, device_id_type=MESH)
        copy.start()
        copies.append(copy)
        return copy

    stage = []
    for s in range(1, nd):
        to = place.other(2, s)
        stage.append(send(p_ref.at[:, :, to[2], :, left], r1a.at[s - 1], place.device(to)))
    for s in range(1, na):
        to = place.other(0, s)
        stage.append(send(p_ref.at[to[0], :, :, :, right], r1b.at[s - 1], place.device(to)))
    kv = [send(dk_ref.at[1], kvr.at[0], place.partner()),
          send(dv_ref.at[1], kvr.at[1], place.partner())]
    for copy in stage:
        copy.wait_recv()

    for i in range(na):
        for j in range(nb):
            total = p_ref[i, j, d, :, left].astype(F32)
            for s in range(nd - 1):
                total = total + r1a[s, i, j].astype(F32)
            t1a[i, j] = total.astype(BF)
    for j in range(nb):
        for i in range(nd):
            total = p_ref[a, j, i, :, right].astype(F32)
            for s in range(na - 1):
                total = total + r1b[s, j, i].astype(F32)
            t1b[i, j] = total.astype(BF)

    stage2 = []
    for s in range(1, na):
        to = place.other(0, s)
        stage2.append(send(t1a.at[to[0]], r2a.at[s - 1], place.device(to)))
    for s in range(1, nd):
        to = place.other(2, s)
        stage2.append(send(t1b.at[to[2]], r2b.at[s - 1], place.device(to)))
    for copy in stage2:
        copy.wait_recv()
    for j in range(nb):
        total = t1a[a, j].astype(F32)
        for s in range(na - 1):
            total = total + r2a[s, j].astype(F32)
        t2[j, :, left] = total.astype(BF)
        total = t1b[d, j].astype(F32)
        for s in range(nd - 1):
            total = total + r2b[s, j].astype(F32)
        t2[j, :, right] = total.astype(BF)
    stage3 = []
    for s in range(1, nb):
        to = place.other(1, s)
        stage3.append(send(t2.at[to[1]], r3.at[s - 1], place.device(to)))

    for copy in kv:
        copy.wait_recv()
    chunk = 128

    def add_part(n, carry):
        at = pl.ds(pl.multiple_of(n * chunk, chunk), chunk)
        dk_out[at, :] = (dk_ref[0, at, :].astype(F32) + kvr[0, at, :].astype(F32)).astype(BF)
        dv_out[at, :] = (dv_ref[0, at, :].astype(F32) + kvr[1, at, :].astype(F32)).astype(BF)
        return carry

    lax.fori_loop(0, dk_out.shape[0] // chunk, add_part, 0)
    for copy in stage3:
        copy.wait_recv()
    total = t2[b].astype(F32)
    for s in range(nb - 1):
        total = total + r3[s].astype(F32)
    dq_out[...] = total
    for copy in copies:
        copy.wait_send()


def reduce(dims, partial, dk, dv):
    na, nb, nd = dims
    rows, width = partial.shape[-2:]
    half = width // 2
    keys, kw = dk.shape[1:]
    count = 2 * (na - 1) + 2 * (nd - 1) + (nb - 1) + 2
    vmem = pl.BlockSpec(memory_space=pltpu.VMEM)
    return pl.pallas_call(
        functools.partial(reduce_kernel, dims),
        name="reduce",
        out_shape=(
            jax.ShapeDtypeStruct((rows, width), F32),
            jax.ShapeDtypeStruct((keys, kw), BF),
            jax.ShapeDtypeStruct((keys, kw), BF),
        ),
        in_specs=[vmem] * 3,
        out_specs=(vmem,) * 3,
        scratch_shapes=[
            pltpu.VMEM((2, keys, kw), BF),
            pltpu.VMEM((max(nd - 1, 1), na, nb, rows, half), BF),
            pltpu.VMEM((max(na - 1, 1), nb, nd, rows, half), BF),
            pltpu.VMEM((na, nb, rows, half), BF),
            pltpu.VMEM((nd, nb, rows, half), BF),
            pltpu.VMEM((max(na - 1, 1), nb, rows, half), BF),
            pltpu.VMEM((max(nd - 1, 1), nb, rows, half), BF),
            pltpu.VMEM((nb, rows, width), BF),
            pltpu.VMEM((max(nb - 1, 1), rows, width), BF),
            pltpu.SemaphoreType.DMA((count,)),
            pltpu.SemaphoreType.DMA((count,)),
        ],
        compiler_params=pltpu.CompilerParams(collective_id=1, has_side_effects=True),
    )(partial, dk, dv)


def local(dims, queries, out_grad, forward_out, lse_shift, key_rows, value_rows):
    members = dims[0] * dims[1] * dims[2]
    rows, width = queries.shape
    keys, kw = key_rows.shape
    total_keys = keys * members * 2
    q, d, aux, k, v = gather(
        dims, total_keys, queries, out_grad, forward_out, lse_shift, key_rows, value_rows)
    dq, dk, dv = attend(
        q.reshape(members * rows, width), d.reshape(members * rows, width), aux,
        k.reshape(2 * keys, kw), v.reshape(2 * keys, kw))
    return reduce(dims, dq.reshape(*dims, rows, width),
                  dk.reshape(2, keys, kw), dv.reshape(2, keys, kw))


def solution(mesh):
    dims = grid_of(mesh.shape["sa"], mesh.shape["sb"])
    spec = P(("sa", "sb"), None)
    return jax.shard_map(functools.partial(local, dims), mesh=mesh, in_specs=(spec,) * 6,
                         out_specs=(spec,) * 3, check_vma=False)
```

```python
import functools
import math

import jax
import jax.numpy as jnp
from jax import lax
from jax.experimental import pallas as pl
from jax.experimental.pallas import tpu as pltpu
from jax.sharding import PartitionSpec as P

QH = 8
KVH = 2
HEAD_DIM = 128
MESH = pl.DeviceIdType.MESH
BF = jnp.bfloat16
F32 = jnp.float32
AXES = ("sa", "sb")


def grid_of(sa, sb):
    inner = 2 ** (int(math.log2(sb)) // 2)
    return sa // 2, sb // inner, inner


class Place:
    def __init__(self, dims):
        self.dims = dims
        sa, sb = lax.axis_index("sa"), lax.axis_index("sb")
        self.core = sa % 2
        self.at = (sa // 2, sb // dims[2], sb % dims[2])

    def other(self, axis, step):
        at = list(self.at)
        at[axis] = (at[axis] + step) % self.dims[axis]
        return tuple(at)

    def back(self, offset):
        return tuple((p + n - o) % n for p, n, o in zip(self.at, self.dims, offset))

    def device(self, at):
        return (at[0] * 2 + self.core, at[1] * self.dims[2] + at[2])

    def partner(self):
        return (self.at[0] * 2 + 1 - self.core, lax.axis_index("sb"))

    def slot(self, at):
        return (at[0] * self.dims[1] + at[1]) * self.dims[2] + at[2]

    def greet(self):
        barrier = pltpu.get_barrier_semaphore()
        peers = [self.partner()]
        for axis in range(3):
            for step in range(1, self.dims[axis]):
                peers.append(self.device(self.other(axis, step)))
        for peer in peers:
            pl.semaphore_signal(barrier, inc=1, device_id=peer, device_id_type=MESH)
        pl.semaphore_wait(barrier, len(peers))


def pieces(x):
    hi = x.astype(BF)
    rest = x - hi.astype(F32)
    mid = rest.astype(BF)
    low = (rest - mid.astype(F32)).astype(BF)
    return hi, mid, low


def relay_sends(dims):
    na, nb, nd = dims
    line, corner = [], []
    for b in range(1, nb):
        line += [((0, b, 0), 2, step) for step in range(1, nd)]
        line += [((0, b, 0), 0, step) for step in range(1, na)]
    for b in range(nb):
        corner += [("x", (0, b, d), 0, s) for d in range(1, nd) for s in range(1, na)]
        corner += [("d", (a, b, 0), 2, s) for a in range(1, na) for s in range(1, nd)]
    return line, corner


def first_sends(dims):
    along = [(1, step) for step in range(1, dims[1])]
    across = [(2, step) for step in range(1, dims[2])] + [(0, step) for step in range(1, dims[0])]
    return along, across


def counts(dims):
    na, nb, nd = dims
    line, corner = relay_sends(dims)
    along, across = first_sends(dims)
    own = len(along) + len(across) + len(line)
    x_diag = sum(1 for c in corner if c[0] == "x")
    gathered = 5 * own + 3 * x_diag + 2 * (len(corner) - x_diag)
    reduced = 2 * (2 * (na - 1) + 2 * (nd - 1) + (nb - 1))
    return gathered, reduced


def whole_kernel(dims, total_keys, tile, q_ref, d_ref, o_ref, lse_ref, k_ref, v_ref,
                 dq_out, dk_out, dv_out,
                 qa, da, xa, aux_ref, ks, va, half, halfr, acc, part, dks, dvs, kvr,
                 r1a, r1b, t1a, t1b, r2a, r2b, t2, r3,
                 send_sem, q_sem, d_sem, x_sem, kv_send, kv_recv, red_send, red_recv):
    na, nb, nd = dims
    members = na * nb * nd
    place = Place(dims)
    pa, pb, pd = place.at
    rows = q_ref.shape[0]
    keys = k_ref.shape[0]
    group = q_ref.shape[1] // KVH
    per_group = QH // KVH
    me = place.slot(place.at)
    scale = 1.0 / math.sqrt(HEAD_DIM)
    place.greet()
    line, corner = relay_sends(dims)
    along, across = first_sends(dims)
    origin = (0, 0, 0)

    partner_copies = []

    def to_partner(src, dst):
        n = len(partner_copies)
        copy = pltpu.make_async_remote_copy(
            src_ref=src, dst_ref=dst, send_sem=kv_send.at[n], recv_sem=kv_recv.at[n],
            device_id=place.partner(), device_id_type=MESH)
        copy.start()
        partner_copies.append(copy)
        return copy

    to_partner(k_ref, ks.at[1])
    to_partner(v_ref, va.at[1])

    def flat(offset):
        return (offset[0] * nb + offset[1]) * nd + offset[2]

    def places(kind, slot, offset):
        if kind == "x":
            return xa.at[slot], x_sem.at[flat(offset)]
        c = int(kind[1])
        buf, sem = (qa, q_sem) if kind[0] == "q" else (da, d_sem)
        return buf.at[c, slot], sem.at[c, flat(offset)]

    started = []

    def send(kind, offset, axis, step):
        slot = place.slot(place.back(offset))
        there = list(offset)
        there[axis] = (there[axis] + step) % dims[axis]
        ref, sem = places(kind, slot, there)
        src = ref
        if offset == origin and kind != "x":
            src = (q_ref if kind[0] == "q" else d_ref).at[:, pl.ds(int(kind[1]) * group, group)]
        copy = pltpu.make_async_remote_copy(
            src_ref=src, dst_ref=ref, send_sem=send_sem.at[len(started)], recv_sem=sem,
            device_id=place.device(place.other(axis, step)), device_id_type=MESH)
        copy.start()
        started.append(copy)

    arrived = set()

    def need(kind, offset):
        if offset == origin or (kind, offset) in arrived:
            return
        arrived.add((kind, offset))
        ref, sem = places(kind, place.slot(place.back(offset)), offset)
        pltpu.make_async_remote_copy(
            src_ref=ref, dst_ref=ref, send_sem=send_sem.at[0], recv_sem=sem,
            device_id=place.partner(), device_id_type=MESH).wait_recv()

    def send_first(kind, directions):
        for axis, step in directions:
            send(kind, origin, axis, step)

    def send_line(kinds):
        for offset, axis, step in line:
            for kind in kinds:
                need(kind, offset)
                send(kind, offset, axis, step)

    def send_corner(kinds):
        for which, offset, axis, step in corner:
            for kind in kinds:
                if (kind[0] == "d") == (which == "d"):
                    need(kind, offset)
                    send(kind, offset, axis, step)

    def need_all(kinds):
        for a in range(na):
            for b in range(nb):
                for d in range(nd):
                    for kind in kinds:
                        need(kind, (a, b, d))

    for kind in ("q0", "d0"):
        send_first(kind, along + across)

    lane = lax.broadcasted_iota(jnp.int32, (rows, HEAD_DIM), 1)
    aux = jnp.zeros((rows, HEAD_DIM), F32)
    for head in range(QH):
        cols = pl.ds(head * HEAD_DIM, HEAD_DIM)
        product = d_ref[:, cols].astype(F32) * o_ref[:, cols].astype(F32)
        delta = jnp.sum(product, axis=1, keepdims=True)
        offset = (lse_ref[:, head:head + 1] + math.log(total_keys)) * (1.0 / scale)
        for at, value in ((0, offset), (3 * QH, delta)):
            for n, piece in enumerate(pieces(value)):
                aux = jnp.where(lane == at + 3 * head + n, piece.astype(F32), aux)
    xa[me, pl.ds(0, rows), :] = aux.astype(BF)
    chunk = 128

    def add_rows(n, total):
        block = k_ref[pl.ds(pl.multiple_of(n * chunk, chunk), chunk), :].astype(F32)
        return total + jnp.sum(block, axis=0, keepdims=True)

    key_sum = lax.fori_loop(0, keys // chunk, add_rows, jnp.zeros((1, KVH * HEAD_DIM), F32))
    row = lax.broadcasted_iota(jnp.int32, (16, HEAD_DIM), 0)
    small = jnp.zeros((16, HEAD_DIM), F32)
    for n, piece in enumerate(pieces(key_sum)):
        for c in range(KVH):
            term = piece[:, c * HEAD_DIM:(c + 1) * HEAD_DIM].astype(F32)
            small = jnp.where(row == 2 * n + c, term, small)
    xa[me, pl.ds(rows, 16), :] = small.astype(BF)
    send_first("x", along + across)
    for kind in ("q1", "d1"):
        send_first(kind, along)
    for c in range(KVH):
        qa[c, me] = q_ref[:, pl.ds(c * group, group)]
        da[c, me] = d_ref[:, pl.ds(c * group, group)]
    va[0] = v_ref[...]
    send_line(("x",))
    send_line(("q0", "d0"))
    send_corner(("x",))
    send_corner(("q0", "d0"))
    for kind in ("q1", "d1"):
        send_first(kind, across)

    need_all(("x",))
    half_sum = jnp.zeros((16, HEAD_DIM), F32)
    for g in range(members):
        half_sum = half_sum + xa[g, pl.ds(rows, 16), :].astype(F32)
        aux_ref[pl.ds(g * rows, rows), :] = xa[g, pl.ds(0, rows), :]
    half[...] = half_sum
    to_partner(half, halfr)
    send_line(("q1", "d1"))
    for copy in partner_copies:
        copy.wait_recv()
    both = half[...] + halfr[...]
    for c in range(KVH):
        cols = pl.ds(c * HEAD_DIM, HEAD_DIM)
        mean = (both[c:c + 1] + both[c + 2:c + 3] + both[c + 4:c + 5]) / total_keys

        def smooth(n, carry):
            at = pl.ds(pl.multiple_of(n * chunk, chunk), chunk)
            ks[0, at, cols] = (k_ref[at, cols].astype(F32) - mean).astype(BF)
            ks[1, at, cols] = (ks[1, at, cols].astype(F32) - mean).astype(BF)
            return carry

        lax.fori_loop(0, keys // chunk, smooth, 0)
    need_all(("q0", "d0"))

    nt = (((1,), (1,)), ((), ()))
    tiles = keys // tile
    key_lane = lax.broadcasted_iota(jnp.int32, (tile, HEAD_DIM), 1)

    def attend(c, side, first):
        cols = pl.ds(c * HEAD_DIM, HEAD_DIM)

        def one(t, carry):
            at = pl.ds(pl.multiple_of(t * tile, tile), tile)
            kt = ks[side, at, cols]
            vt = va[side, at, cols]
            aux_all = aux_ref[...]
            dk = jnp.zeros((tile, HEAD_DIM), F32)
            dv = jnp.zeros((tile, HEAD_DIM), F32)
            for g in range(per_group):
                head_cols = pl.ds(g * HEAD_DIM, HEAD_DIM)
                heads_q = qa[c, :, :, head_cols].reshape(members * rows, HEAD_DIM)
                heads_d = da[c, :, :, head_cols].reshape(members * rows, HEAD_DIM)
                low = 3 * (c * per_group + g)
                minus_s = jnp.where((key_lane >= low) & (key_lane < low + 3), -1.0, 0.0)
                low = low + 3 * QH
                minus_d = jnp.where((key_lane >= low) & (key_lane < low + 3), -1.0, 0.0)
                s = lax.dot_general(jnp.concatenate([kt, minus_s.astype(BF)], 1),
                                    jnp.concatenate([heads_q, aux_all], 1), nt,
                                    preferred_element_type=F32)
                dp = lax.dot_general(jnp.concatenate([vt, minus_d.astype(BF)], 1),
                                     jnp.concatenate([heads_d, aux_all], 1), nt,
                                     preferred_element_type=F32)
                prob = jnp.exp2(s * (scale * math.log2(math.e)))
                dv = dv + jnp.dot(prob.astype(BF), heads_d, preferred_element_type=F32)
                ds = (prob * dp).astype(BF)
                dk = dk + jnp.dot(ds, heads_q, preferred_element_type=F32)
                acc[:, head_cols] += lax.dot_general(
                    ds, kt, (((0,), (0,)), ((), ())), preferred_element_type=F32)
            dks[c, side, at, :] = (dk * scale).astype(BF)
            dvs[c, side, at, :] = dv.astype(BF)
            return carry

        if first:
            acc[...] = jnp.zeros(acc.shape, F32)
        lax.fori_loop(0, tiles, one, 0)

    def finish(c):
        part[c] = (acc[...] * scale).reshape(na, nb, nd, rows, group).astype(BF)

    mid = group // 2
    left, right = pl.ds(0, mid), pl.ds(mid, mid)
    reduced = []

    def red(src, dst, to):
        n = len(reduced)
        copy = pltpu.make_async_remote_copy(
            src_ref=src, dst_ref=dst, send_sem=red_send.at[n], recv_sem=red_recv.at[n],
            device_id=place.device(to), device_id_type=MESH)
        copy.start()
        reduced.append(copy)
        return copy

    def stage1(c):
        stage = []
        for s in range(1, nd):
            to = place.other(2, s)
            stage.append(red(part.at[c, :, :, to[2], :, left], r1a.at[c, s - 1], to))
        for s in range(1, na):
            to = place.other(0, s)
            stage.append(red(part.at[c, to[0], :, :, :, right], r1b.at[c, s - 1], to))
        return stage

    def stage2(c, stage):
        for copy in stage:
            copy.wait_recv()
        for i in range(na):
            for j in range(nb):
                total = part[c, i, j, pd, :, left].astype(F32)
                for s in range(nd - 1):
                    total = total + r1a[c, s, i, j].astype(F32)
                t1a[c, i, j] = total.astype(BF)
        for j in range(nb):
            for i in range(nd):
                total = part[c, pa, j, i, :, right].astype(F32)
                for s in range(na - 1):
                    total = total + r1b[c, s, j, i].astype(F32)
                t1b[c, i, j] = total.astype(BF)
        stage = []
        for s in range(1, na):
            to = place.other(0, s)
            stage.append(red(t1a.at[c, to[0]], r2a.at[c, s - 1], to))
        for s in range(1, nd):
            to = place.other(2, s)
            stage.append(red(t1b.at[c, to[2]], r2b.at[c, s - 1], to))
        return stage

    def stage3(c, stage):
        for copy in stage:
            copy.wait_recv()
        for j in range(nb):
            total = t1a[c, pa, j].astype(F32)
            for s in range(na - 1):
                total = total + r2a[c, s, j].astype(F32)
            t2[c, j, :, left] = total.astype(BF)
            total = t1b[c, pd, j].astype(F32)
            for s in range(nd - 1):
                total = total + r2b[c, s, j].astype(F32)
            t2[c, j, :, right] = total.astype(BF)
        stage = []
        for s in range(1, nb):
            to = place.other(1, s)
            stage.append(red(t2.at[c, to[1]], r3.at[c, s - 1], to))
        return stage

    def last(c, stage):
        for copy in stage:
            copy.wait_recv()
        total = t2[c, pb].astype(F32)
        for s in range(nb - 1):
            total = total + r3[c, s].astype(F32)
        dq_out[:, pl.ds(c * group, group)] = total

    kv = []
    for c in range(KVH):
        attend(c, 1, True)
        kv.append(to_partner(dks.at[c, 1], kvr.at[c, 0]))
        kv.append(to_partner(dvs.at[c, 1], kvr.at[c, 1]))
        if c == 0:
            send_corner(("q1", "d1"))
        else:
            stage = stage2(0, stage)
        attend(c, 0, False)
        finish(c)
        if c == 0:
            stage = stage1(0)
            need_all(("q1", "d1"))
    ending = stage1(1)
    stage = stage3(0, stage)

    for copy in kv:
        copy.wait_recv()

    def add_part(n, carry):
        at = pl.ds(pl.multiple_of(n * chunk, chunk), chunk)
        for c in range(KVH):
            cols = pl.ds(c * HEAD_DIM, HEAD_DIM)
            for out, mine, where in ((dk_out, dks, 0), (dv_out, dvs, 1)):
                out[at, cols] = (mine[c, 0, at, :].astype(F32)
                                 + kvr[c, where, at, :].astype(F32)).astype(BF)
        return carry

    lax.fori_loop(0, keys // chunk, add_part, 0)
    ending = stage2(1, ending)
    last(0, stage)
    ending = stage3(1, ending)
    last(1, ending)
    for copy in started + partner_copies + reduced:
        copy.wait_send()


def local(dims, q, d, o, lse, k, v):
    na, nb, nd = dims
    members = na * nb * nd
    rows, width = q.shape
    keys, kw = k.shape
    group, mid = width // KVH, width // KVH // 2
    tile = min(512, keys)
    gathered, reduced = counts(dims)
    vmem = pl.BlockSpec(memory_space=pltpu.VMEM)
    ma, mb, md = max(na - 1, 1), max(nb - 1, 1), max(nd - 1, 1)
    sem = pltpu.SemaphoreType.DMA
    return pl.pallas_call(
        functools.partial(whole_kernel, dims, keys * members * 2, tile),
        name="whole",
        out_shape=(
            jax.ShapeDtypeStruct((rows, width), F32),
            jax.ShapeDtypeStruct((keys, kw), BF),
            jax.ShapeDtypeStruct((keys, kw), BF),
        ),
        in_specs=[vmem] * 6,
        out_specs=(vmem,) * 3,
        scratch_shapes=[
            pltpu.VMEM((KVH, members, rows, group), BF),
            pltpu.VMEM((KVH, members, rows, group), BF),
            pltpu.VMEM((members, rows + 16, HEAD_DIM), BF),
            pltpu.VMEM((members * rows, HEAD_DIM), BF),
            pltpu.VMEM((2, keys, kw), BF),
            pltpu.VMEM((2, keys, kw), BF),
            pltpu.VMEM((16, HEAD_DIM), F32),
            pltpu.VMEM((16, HEAD_DIM), F32),
            pltpu.VMEM((members * rows, group), F32),
            pltpu.VMEM((KVH, na, nb, nd, rows, group), BF),
            pltpu.VMEM((KVH, 2, keys, HEAD_DIM), BF),
            pltpu.VMEM((KVH, 2, keys, HEAD_DIM), BF),
            pltpu.VMEM((KVH, 2, keys, HEAD_DIM), BF),
            pltpu.VMEM((KVH, md, na, nb, rows, mid), BF),
            pltpu.VMEM((KVH, ma, nb, nd, rows, mid), BF),
            pltpu.VMEM((KVH, na, nb, rows, mid), BF),
            pltpu.VMEM((KVH, nd, nb, rows, mid), BF),
            pltpu.VMEM((KVH, ma, nb, rows, mid), BF),
            pltpu.VMEM((KVH, md, nb, rows, mid), BF),
            pltpu.VMEM((KVH, nb, rows, group), BF),
            pltpu.VMEM((KVH, mb, rows, group), BF),
            sem((gathered,)),
            sem((KVH, members)),
            sem((KVH, members)),
            sem((members,)),
            sem((3 + 2 * KVH,)),
            sem((3 + 2 * KVH,)),
            sem((reduced,)),
            sem((reduced,)),
        ],
        compiler_params=pltpu.CompilerParams(
            collective_id=0, has_side_effects=True, vmem_limit_bytes=60 * 1024 * 1024),
    )(q, d, o, lse, k, v)


def solution(mesh):
    dims = grid_of(mesh.shape["sa"], mesh.shape["sb"])
    spec = P(("sa", "sb"), None)
    return jax.shard_map(functools.partial(local, dims), mesh=mesh, in_specs=(spec,) * 6,
                         out_specs=(spec,) * 3, check_vma=False)
```
